32 devices in a mesh: day: 8 (over z, x), blk: 4 (over y, core).
Axes of the slice: x: 2, y: 2, z: 4, core: 2. Of those that a mesh axis runs over, the one named last changes fastest.
Arguments:
- diag_blocks: float32 [16, 2560, 2560], P('day', 'blk'), may hold values from -1 to 3, as said below
- off_blocks: float32 [16, 2560, 2560], P('day', 'blk'), may hold values from -1 to 1
- leakage: float32 [16, 2560], P('day', 'blk'), may hold values from 0.001 to 0.3
- obs_count: int32 [16], P('day'), may hold values from 1 to 1024, 8192 in all
- obs_triangle: int32 [16, 1024], P('day', 'blk'), may hold values from 0 to 5115
- obs_bary: float32 [3, 16, 1024], P(None, 'day', 'blk'), may hold values from 0.05 to 1
- obs_prec: float32 [16, 1024], P('day', 'blk'), may hold values from 0.3 to 3
- obs_value: float32 [16, 1024], P('day', 'blk'), may hold values from -6 to 6
- covariates: float32 [64, 16, 1024], P(None, 'day', 'blk'), may hold values from -0.09375 to 0.09375
- triangles: int32 [3, 5116], replicated, may hold values from 0 to 2559
- prior_prec: float32 [64], replicated, may hold values from 0.5 to 2
- probes: float32 [15, 16, 2560], P(None, 'day', 'blk'), may hold values from -6 to 6
- probes_cov: float32 [15, 64], replicated, may hold values from -6 to 6
Outputs:
- step_field: float32 [16, 16, 2560], P(None, 'day', 'blk')
- step_cov: float32 [16, 64], replicated
The draws below stay inside these ranges and needn't reach their ends.
Inputs may be any that keep to these rules, and one draw needn't show every extreme that they name: Every block diag_blocks[t] is symmetric, and the whole precision made of diag_blocks and off_blocks is positive definite. Slots 0 to obs_count[t] - 1 of day t hold observations, the others are empty; the counts sum to 8192.
All inputs are finite; a program needn't handle non-finite values. No bound on the sum of `obs_count` on one device may be relied on, other than what follows from the above.
Results may differ from the reference program's by a relative error of at most 0.0002.
Values sent between devices are 32-bit elements; how exact they have to be, the bound alone decides.
A program may use at most 192 MiB of HBM per device.

```python
import math
import jax
import jax.numpy as jnp
import numpy as np
from jax import lax

S = 2560
COV = 64
PROBES = 15
ITERS = 3
OBS_CAP = 1024
DAYS = 16
NTRI = 5116


def draw_diag_blocks(key, part):
    first_key, second_key = jax.random.split(jax.random.fold_in(key, 11))
    raw_entries = jax.random.normal(first_key, (DAYS, S, S), jnp.float32)
    symmetric = (raw_entries + jnp.swapaxes(raw_entries, 1, 2)) * (0.3 / math.sqrt(2.0 * S))
    levels = jax.random.uniform(second_key, (DAYS, S), jnp.float32, 1.2, 2.2)
    return symmetric + levels[:, :, None] * jnp.eye(S, dtype=jnp.float32)


def draw_off_blocks(key, part):
    entry_key = jax.random.fold_in(key, 23)
    raw_entries = jax.random.normal(entry_key, (DAYS, S, S), jnp.float32)
    return raw_entries * (0.125 / math.sqrt(S))


def with_ends(array, key, low, top_value):
    place = [jax.random.randint(jax.random.fold_in(key, axis), (), 0, length) for axis, length in enumerate(array.shape)]
    main_axis = array.shape.index(max(array.shape))
    next_to = place[:main_axis] + [(place[main_axis] + 1) % array.shape[main_axis]] + place[main_axis + 1:]
    return array.at[tuple(place)].set(low).at[tuple(next_to)].set(top_value)


def steps_of(rng, dims, pieces, low, top_value):
    def one(position, blocks):
        heights = jax.random.uniform(jax.random.fold_in(jax.random.fold_in(rng, 6), position), (blocks,), jnp.float32, low / len(pieces), top_value / len(pieces))
        return jnp.repeat(jnp.exp(heights), dims[position] // blocks).reshape((-1,) + (1,) * (len(dims) - position - 1))

    loudness = one(*pieces[0])
    for cut in pieces[1:]:
        loudness = loudness * one(*cut)
    return loudness


def profile(amount, total, reach, lean):
    loads = [(1 << 20) // math.isqrt(rank ** lean) + 1 for rank in range(2, amount + 1)]
    spare, holding = total - reach - (amount - 1), [1] * (amount - 1)
    while spare > 0:
        candidates = [i for i in range(amount - 1) if holding[i] < reach]
        mass, budget = sum([loads[i] for i in candidates]), spare
        for i in candidates:
            extra = min(reach - holding[i], max(1, budget * loads[i] // mass), spare)
            holding[i] = holding[i] + extra
            spare = spare - extra
    return np.array([reach] + holding)


def uneven_parts(stream_key, number_of, total, bound, slope):
    if number_of == 2:
        one = jax.random.randint(stream_key, (), max(1, total - bound), min(bound, total - 1) + 1)
        return jnp.stack([one, total - one])
    lengths = jnp.asarray(profile(number_of, total, bound, slope), jnp.int32)
    pairs = (number_of - 1) // 2
    source_of, sink = lengths[1:1 + 2 * pairs:2], lengths[2:2 + 2 * pairs:2]
    margin = jnp.minimum(source_of - 1, bound - sink)
    shifted = jax.random.randint(jax.random.fold_in(stream_key, 1), (pairs,), 0, 1 << 20) % (margin + 1)
    lengths = lengths.at[1:1 + 2 * pairs:2].set(source_of - shifted).at[2:2 + 2 * pairs:2].set(sink + shifted)
    return lengths[jax.random.permutation(jax.random.fold_in(stream_key, 2), number_of)]


def noise(stream_key, shape, deviation, bound, cuts=(), kind=jnp.bfloat16):
    gain = steps_of(stream_key, shape, cuts, -0.22, 0.18) if cuts else 1.0
    entries = jax.random.normal(stream_key, shape, jnp.float32) * deviation * gain
    return jnp.minimum(jnp.maximum(entries, -bound), bound).astype(kind)


def setup_inputs(seed: int = 0) -> dict:
    keys = jax.random.split(jax.random.key(seed), 14)
    return {
        "diag_blocks": draw_diag_blocks(jax.random.fold_in(keys[13], 71), 0),
        "off_blocks": draw_off_blocks(jax.random.fold_in(keys[13], 71), 0),
        "leakage": jnp.clip(jnp.exp(math.log(0.3) - 5.7037825 * jax.random.uniform(keys[2], (DAYS, S), jnp.float32) ** steps_of(keys[2], (DAYS, S), ((0, 8), (1, 4)), -0.2, 0.2)), 0.001, 0.3),
        "obs_count": uneven_parts(keys[3], DAYS, DAYS * OBS_CAP // 2, OBS_CAP, 2).astype(jnp.int32),
        "obs_triangle": with_ends(jax.random.randint(keys[4], (DAYS, OBS_CAP), 0, NTRI), jax.random.fold_in(keys[4], 1), 0, NTRI - 1).astype(jnp.int32),
        "obs_bary": jnp.clip(jnp.exp(math.log(1.0) - 2.9957323 * jax.random.uniform(keys[5], (3, DAYS, OBS_CAP), jnp.float32) ** steps_of(keys[5], (3, DAYS, OBS_CAP), ((1, 8), (2, 4)), -0.2, 0.2)), 0.05, 1.0),
        "obs_prec": jnp.clip(jnp.exp(math.log(3.0) - 2.3025851 * jax.random.uniform(keys[6], (DAYS, OBS_CAP), jnp.float32) ** steps_of(keys[6], (DAYS, OBS_CAP), ((0, 8), (1, 4)), -0.2, 0.2)), 0.3, 3.0),
        "obs_value": noise(keys[7], (DAYS, OBS_CAP), 1.0, 6.0, ((0, 8), (1, 4)), jnp.float32),
        "covariates": noise(keys[8], (COV, DAYS, OBS_CAP), (DAYS * OBS_CAP // 4) ** -0.5, 0.09375, ((1, 8), (2, 4)), jnp.float32),
        "triangles": with_ends(jax.random.randint(keys[9], (3, NTRI), 0, S), jax.random.fold_in(keys[9], 1), 0, S - 1).astype(jnp.int32),
        "prior_prec": jnp.clip(jnp.exp(jax.random.uniform(keys[10], (COV,), jnp.float32, math.log(0.5), math.log(2.0))), 0.5, 2.0),
        "probes": noise(keys[11], (PROBES, DAYS, S), 1.0, 6.0, ((1, 8), (2, 4)), jnp.float32),
        "probes_cov": noise(keys[12], (PROBES, COV), 1.0, 6.0, (), jnp.float32),
    }


def spread(values, flat_ids, segments):
    leading = values.shape[0]
    summed = jax.ops.segment_sum(values.reshape(leading, -1).T, flat_ids, num_segments=segments)
    return summed.T


def observation_setup(obs_count, obs_triangle, obs_bary, obs_prec, triangles):
    slot_index = lax.broadcasted_iota(jnp.int32, obs_triangle.shape, 1)
    slot_weight = jnp.where(slot_index < obs_count[:, None], obs_prec, jnp.zeros_like(obs_prec))
    vertices = triangles[:, obs_triangle].astype(jnp.int32)
    day_index = lax.broadcasted_iota(jnp.int32, vertices.shape, 1)
    flat_ids = (vertices + S * day_index).reshape(-1).astype(jnp.int32)
    barycentric = obs_bary / jnp.sum(obs_bary, axis=0, keepdims=True)
    return flat_ids, barycentric, slot_weight


def apply_hessian(direction, direction_cov, diag_blocks, off_blocks, flat_ids, barycentric, slot_weight, covariates, prior_prec):
    rhs_count = direction.shape[0]
    exact = lax.Precision.HIGHEST
    diagonal_terms = jnp.einsum('tij,rtj->rti', diag_blocks, direction, precision=exact)
    ahead_terms = jnp.einsum('tij,rtj->rti', off_blocks[:-1], direction[:, 1:], precision=exact)
    behind_terms = jnp.einsum('tji,rtj->rti', off_blocks[:-1], direction[:, :-1], precision=exact)
    empty_day = jnp.zeros((rhs_count, 1, S), jnp.float32)
    coupled = diagonal_terms + jnp.concatenate([ahead_terms, empty_day], axis=1) + jnp.concatenate([empty_day, behind_terms], axis=1)
    picked = direction.reshape(rhs_count, -1)[:, flat_ids].reshape((rhs_count,) + barycentric.shape)
    predictor = jnp.sum(barycentric[None] * picked, axis=1) + jnp.einsum('ctj,rc->rtj', covariates, direction_cov, precision=exact)
    weighted = slot_weight[None] * predictor
    obs_terms = spread(barycentric[None] * weighted[:, None], flat_ids, DAYS * S).reshape(rhs_count, DAYS, S)
    image_cov = jnp.einsum('ctj,rtj->rc', covariates, weighted, precision=exact) + prior_prec[None] * direction_cov
    return coupled + obs_terms, image_cov


def precondition(residual, decays, dominant):
    start = jnp.zeros((residual.shape[0], S), jnp.float32)

    def forward(running, pair):
        value_day, decay_day = pair
        running = value_day + decay_day[None] * running
        return running, running

    unused, lowered = lax.scan(forward, start, (jnp.swapaxes(residual, 0, 1), decays))
    scaled = lowered / dominant[:, None, :]
    decay_next = jnp.concatenate([decays[1:], jnp.zeros((1, S), jnp.float32)], axis=0)

    def backward(running, pair):
        value_day, decay_day = pair
        running = value_day + decay_day[None] * running
        return running, running

    unused, raised = lax.scan(backward, start, (scaled, decay_next), reverse=True)
    return jnp.swapaxes(raised, 0, 1)


def reference(diag_blocks, off_blocks, leakage, obs_count, obs_triangle, obs_bary, obs_prec, obs_value, covariates, triangles, prior_prec, probes, probes_cov):
    flat_ids, barycentric, slot_weight = observation_setup(obs_count, obs_triangle, obs_bary, obs_prec, triangles)
    decays = 1.0 - leakage
    dominant = jnp.diagonal(diag_blocks, axis1=1, axis2=2)
    weighted_value = slot_weight * obs_value
    grad_field = spread((barycentric * weighted_value[None])[None], flat_ids, DAYS * S).reshape(1, DAYS, S)
    grad_cov = jnp.einsum('ctj,tj->c', covariates, weighted_value, precision=lax.Precision.HIGHEST)
    residual = jnp.concatenate([grad_field, probes], axis=0)
    residual_cov = jnp.concatenate([grad_cov[None], probes_cov], axis=0)
    solution = jnp.zeros_like(residual)
    solution_cov = jnp.zeros_like(residual_cov)
    preconditioned = precondition(residual, decays, dominant)
    direction = preconditioned
    direction_cov = residual_cov
    norm_now = jnp.sum(residual * preconditioned, axis=(1, 2)) + jnp.sum(residual_cov * residual_cov, axis=1)
    for iteration in range(ITERS):
        image, image_cov = apply_hessian(direction, direction_cov, diag_blocks, off_blocks, flat_ids, barycentric, slot_weight, covariates, prior_prec)
        curvature = jnp.sum(direction * image, axis=(1, 2)) + jnp.sum(direction_cov * image_cov, axis=1)
        step_length = norm_now / curvature
        solution = solution + step_length[:, None, None] * direction
        solution_cov = solution_cov + step_length[:, None] * direction_cov
        if iteration + 1 < ITERS:
            residual = residual - step_length[:, None, None] * image
            residual_cov = residual_cov - step_length[:, None] * image_cov
            preconditioned = precondition(residual, decays, dominant)
            norm_next = jnp.sum(residual * preconditioned, axis=(1, 2)) + jnp.sum(residual_cov * residual_cov, axis=1)
            conjugacy = norm_next / norm_now
            direction = preconditioned + conjugacy[:, None, None] * direction
            direction_cov = residual_cov + conjugacy[:, None] * direction_cov
            norm_now = norm_next
    return solution, solution_cov
```

```python
import functools
import jax
import jax.numpy as jnp
from jax import lax
from jax.experimental import pallas as pl
from jax.experimental.pallas import tpu as pltpu
from jax.sharding import PartitionSpec as P

ITERS = 3
COLS = 256
CHUNK = 64
SLOTS = 8
MESH = pl.DeviceIdType.MESH
F32 = jnp.float32
BF16 = jnp.bfloat16


def split(x):
    hi = x.astype(BF16)
    return hi, (x - hi.astype(F32)).astype(BF16)


def nn(a, b):
    return jnp.dot(a, b, preferred_element_type=F32)


def nt(a, b, precision=None):
    return lax.dot_general(
        a, b, (((1,), (1,)), ((), ())), preferred_element_type=F32, precision=precision
    )


def kernel(
    D, B, R, dl, n, J, C,
    diag, off, vert, bary, cov, slotw, wval, leak, probes, pcov, prior,
    field_out, cov_out,
    mhi, mlo, ahi, alo, stage, stage_sem,
    dacc, own_dom, leak_all, dom_all, g_snd, g_rcv, gc_snd, gc_rcv, gcd_snd, gcd_rcv,
    x_snd, x_rcv, resid, pre, pre_rcv, npart, n_rcv, ncol, nb_rcv, pre_own, pre_full,
    dirs, dhl, ohl, part, behind, ahead, p_snd, p_rcv, q_snd, q_rcv, cc, cc_b, cs, cc_d, stepd,
    sem_blk, sem_day, sem_next,
):
    S = n * B
    T = D * dl
    Rd = R // D
    me_d = lax.axis_index("day")
    me_b = lax.axis_index("blk")

    def at_blk(k):
        return lax.rem(me_b + k, B)

    def at_day(k):
        return lax.rem(me_d + k, D)

    def start_all(copies):
        for c in copies:
            c.start()

    def wait_all(copies):
        for c in copies:
            c.wait()

    def to_blk(row, src, dst):
        return [
            pltpu.make_async_remote_copy(
                src_ref=src(at_blk(k)), dst_ref=dst(me_b),
                send_sem=sem_blk.at[0, row, k], recv_sem=sem_blk.at[1, row, k],
                device_id={"blk": at_blk(k)}, device_id_type=MESH,
            )
            for k in range(1, B)
        ]

    def to_day(row, src, dst):
        return [
            pltpu.make_async_remote_copy(
                src_ref=src(at_day(k)), dst_ref=dst(me_d),
                send_sem=sem_day.at[0, row, k], recv_sem=sem_day.at[1, row, k],
                device_id={"day": at_day(k)}, device_id_type=MESH,
            )
            for k in range(1, D)
        ]

    def to_next(row, src, dst):
        return [
            pltpu.make_async_remote_copy(
                src_ref=src(at_blk(k)), dst_ref=dst(me_b),
                send_sem=sem_next.at[0, row, k], recv_sem=sem_next.at[1, row, k],
                device_id={"day": at_day(1), "blk": at_blk(k)}, device_id_type=MESH,
            )
            for k in range(B)
        ]

    def load(mat, q, slot):
        return pltpu.make_async_copy(
            mat.at[pl.ds(pl.multiple_of(q * CHUNK, CHUNK), CHUNK)], stage.at[slot], stage_sem.at[slot]
        )

    total = dl * n // CHUNK
    per_day = n // CHUNK
    for s in range(min(SLOTS, total)):
        load(diag, s, s).start()

    barrier = pltpu.get_barrier_semaphore()
    for k in range(1, B):
        pl.semaphore_signal(barrier, inc=1, device_id={"blk": at_blk(k)}, device_id_type=MESH)
        pl.semaphore_signal(
            barrier, inc=1, device_id={"day": at_day(D - 1), "blk": at_blk(k)}, device_id_type=MESH
        )
    for k in range(1, D):
        pl.semaphore_signal(barrier, inc=1, device_id={"day": at_day(k)}, device_id_type=MESH)

    for t in range(dl):
        v = vert[t]
        b = bary[t]

        def build(c, carry):
            cols = pl.ds(pl.multiple_of(c * COLS, COLS), COLS)
            lane = lax.broadcasted_iota(jnp.int32, (J, COLS), 1) + c * COLS
            acc = jnp.zeros((J, COLS), F32)
            for k in range(3):
                acc = acc + jnp.where(v[:, k : k + 1] == lane, b[:, k : k + 1], 0.0)
            hi, lo = split(acc)
            ahi[t, :, cols] = hi
            alo[t, :, cols] = lo
            return carry

        lax.fori_loop(0, S // COLS, build, 0)

    pl.semaphore_wait(barrier, 2 * (B - 1) + D - 1)

    gc = jnp.zeros((8, C), F32)
    for t in range(dl):
        w8 = jnp.broadcast_to(wval[t], (8, J))
        gc = gc + nt(w8, cov[t], lax.Precision.HIGHEST)
        whi, wlo = split(w8)
        w2 = jnp.concatenate([whi.astype(F32), wlo.astype(F32)], axis=0).astype(BF16)

        def grad(c, carry):
            cols = pl.ds(pl.multiple_of(c * COLS, COLS), COLS)
            g = nn(w2, ahi[t, :, cols])
            part[t, 0:8, cols] = g[:8] + g[8:] + nn(w2, alo[t, :, cols])[:8]
            return carry

        lax.fori_loop(0, S // COLS, grad, 0)
        for j in range(B):
            g_snd[j, t] = part[t, 0:8, j * n : (j + 1) * n]
    gc_snd[...] = jnp.zeros_like(gc_snd)
    gc_snd[:, :C] = gc
    cc[...] = jnp.zeros_like(cc)
    first = to_blk(0, lambda j: g_snd.at[j], lambda m: g_rcv.at[m])
    first += to_blk(1, lambda j: gc_snd, lambda m: gc_rcv.at[m])
    first_leak = to_day(0, lambda g: leak, lambda m: leak_all.at[m])
    start_all(first + first_leak)
    g_rcv[me_b] = g_snd[me_b]
    gc_rcv[me_b] = gc_snd[...]
    leak_all[me_d] = leak[...]

    def convert(mat, base, want_diagonal):
        def one(q, carry):
            slot = lax.rem(q, SLOTS)
            load(mat, q, slot).wait()
            x = stage[slot]
            hi, lo = split(x)
            rows = pl.ds(pl.multiple_of(base + q * CHUNK, CHUNK), CHUNK)
            mhi[rows] = hi
            mlo[rows] = lo
            if want_diagonal:
                first_row = me_b * n + lax.rem(q, per_day) * CHUNK
                gap = lax.broadcasted_iota(jnp.int32, (CHUNK, S), 1) - lax.broadcasted_iota(
                    jnp.int32, (CHUNK, S), 0
                )
                picked = jnp.where(gap == first_row, x, 0.0)
                t = q // per_day
                dacc[t] = dacc[t] + jnp.sum(picked.reshape(CHUNK // 8, 8, S), axis=0)

            @pl.when(q + SLOTS < total)
            def _():
                load(mat, q + SLOTS, slot).start()

            return carry

        lax.fori_loop(0, total, one, 0)

    dacc[...] = jnp.zeros_like(dacc)
    convert(diag, 0, True)
    for s in range(min(SLOTS, total)):
        load(off, s, s).start()
    for t in range(dl):
        row = jnp.sum(dacc[t], axis=0, keepdims=True)
        acc = row[:, :n]
        for j in range(1, B):
            acc = acc + row[:, j * n : (j + 1) * n]
        own_dom[t : t + 1] = acc
    first_dom = to_day(1, lambda g: own_dom, lambda m: dom_all.at[m])
    start_all(first_dom)
    dom_all[me_d] = own_dom[...]

    wait_all(first)
    g_own = jnp.sum(g_rcv[...], axis=0)
    gcd_snd[...] = jnp.sum(gc_rcv[...], axis=0)
    is_first = lax.broadcasted_iota(jnp.int32, (R, 1), 0) == 0
    for t in range(dl):
        r = jnp.where(is_first, jnp.broadcast_to(g_own[t, 0:1], (R, n)), probes[t])
        for g in range(D):
            x_snd[g, t] = r[g * Rd : (g + 1) * Rd]
    move = to_day(2, lambda g: x_snd.at[g], lambda m: x_rcv.at[0, m])
    move += to_day(3, lambda g: gcd_snd, lambda m: gcd_rcv.at[m])
    start_all(move)
    x_rcv[0, me_d] = x_snd[me_d]
    gcd_rcv[me_d] = gcd_snd[...]
    convert(off, dl * n, False)
    wait_all(first_leak + first_dom + move)
    gcov = jnp.sum(gcd_rcv[...], axis=0)[0:1, :C]
    resid_cov = jnp.where(is_first, jnp.broadcast_to(gcov, (R, C)), pcov[...])
    resid[...] = x_rcv[0]
    pre[T] = jnp.zeros((Rd, n), F32)

    live = jnp.where(me_d == D - 1, 0.0, 1.0).astype(F32)
    norm_now = None
    sol_cov = jnp.zeros((R, C), F32)
    dir_cov = None
    row_day = 4
    row_blk = 2
    for it in range(ITERS):
        running = jnp.zeros((Rd, n), F32)
        for t in range(T):
            decay = 1.0 - leak_all[t // dl, t % dl : t % dl + 1]
            running = resid[t // dl, t % dl] + decay * running
            pre[t] = running / dom_all[t // dl, t % dl : t % dl + 1]
        running = pre[T - 1]
        norm_part = resid[D - 1, dl - 1] * running
        for t in range(T - 2, -1, -1):
            u = t + 1
            decay = 1.0 - leak_all[u // dl, u % dl : u % dl + 1]
            running = pre[t] + decay * running
            pre[t] = running
            norm_part = norm_part + resid[t // dl, t % dl] * running
        npart[...] = jnp.broadcast_to(jnp.sum(norm_part, axis=1, keepdims=True), (Rd, 128))
        back = to_day(
            row_day, lambda g: pre.at[pl.ds(g * dl, dl + 1)], lambda m: pre_rcv.at[it, m]
        )
        back += to_day(row_day + 1, lambda g: npart, lambda m: n_rcv.at[it, m])
        start_all(back)
        for t in range(dl + 1):
            pre_rcv[it, me_d, t] = pre[me_d * dl + t]
        n_rcv[it, me_d] = npart[...]
        wait_all(back)
        for g in range(D):
            for t in range(dl + 1):
                pre_own[t, g * Rd : (g + 1) * Rd] = pre_rcv[it, g, t]
            ncol[g * Rd : (g + 1) * Rd] = n_rcv[it, g]
        spread_out = to_blk(row_blk, lambda j: pre_own, lambda m: pre_full.at[it, m])
        spread_out += to_blk(row_blk + 1, lambda j: ncol, lambda m: nb_rcv.at[it, m])
        start_all(spread_out)
        pre_full[it, me_b] = pre_own[...]
        nb_rcv[it, me_b] = ncol[...]
        wait_all(spread_out)
        norm_next = jnp.sum(nb_rcv[it], axis=0)[:, 0:1] + jnp.sum(
            resid_cov * resid_cov, axis=1, keepdims=True
        )
        if it == 0:
            dir_cov = resid_cov
        else:
            beta = norm_next / norm_now
            dir_cov = resid_cov + beta * dir_cov
        norm_now = norm_next
        for j in range(B):
            for t in range(dl + 1):
                d = pre_full[it, j, t]
                if it > 0:
                    d = d + beta * dirs[it - 1, j, t]
                dirs[it, j, t] = d
                hi, lo = split(d)
                dhl[t, 0:R, j * n : (j + 1) * n] = hi
                dhl[t, R : 2 * R, j * n : (j + 1) * n] = lo
        for t in range(dl):
            d = dirs[it, me_b, t]
            hi, lo = split(d)
            ohl[t, 0:R] = hi
            ohl[t, R : 2 * R] = lo

        curve = jnp.zeros((R, 1), F32)
        cov_terms = jnp.zeros((R, C), F32)
        for t in range(dl):
            both = nt(dhl[t], ahi[t])
            predictor = both[:R] + both[R:] + nt(dhl[t, 0:R], alo[t])
            predictor = predictor + jnp.dot(
                dir_cov, cov[t], preferred_element_type=F32, precision=lax.Precision.HIGHEST
            )
            weighted = slotw[t] * predictor
            cov_terms = cov_terms + nt(weighted, cov[t], lax.Precision.HIGHEST)
            whi, wlo = split(weighted)
            w2 = jnp.concatenate([whi, wlo], axis=0)

            def columns(c, carry):
                cols = pl.ds(pl.multiple_of(c * COLS, COLS), COLS)
                rows = slice(t * n, (t + 1) * n)
                orows = slice((dl + t) * n, (dl + t + 1) * n)
                dv = ohl[t]
                x = nn(dv, mhi[rows, cols]) + nn(w2, ahi[t, :, cols])
                y = nn(dv[:R], mlo[rows, cols]) + nn(whi, alo[t, :, cols])
                part[t, :, cols] = x[:R] + x[R:] + y
                x = nn(dv, mhi[orows, cols])
                behind[t, :, cols] = x[:R] + x[R:] + nn(dv[:R], mlo[orows, cols])
                return carry

            lax.fori_loop(0, S // COLS, columns, 0)
            x = nt(dhl[t + 1], mhi[(dl + t) * n : (dl + t + 1) * n])
            ahead[t] = x[:R] + x[R:] + nt(dhl[t + 1, 0:R], mlo[(dl + t) * n : (dl + t + 1) * n])
            curve = curve + jnp.sum(ahead[t] * dirs[it, me_b, t], axis=1, keepdims=True)
        for j in range(B):
            piece = slice(j * n, (j + 1) * n)
            for t in range(dl):
                p = part[t, :, piece]
                if t > 0:
                    p = p + behind[t - 1, :, piece]
                p_snd[j, t] = p
                curve = curve + jnp.sum(p * dirs[it, j, t], axis=1, keepdims=True)
            q = behind[dl - 1, :, piece] * live
            q_snd[j] = q
            curve = curve + jnp.sum(q * dirs[it, j, dl], axis=1, keepdims=True)
        curve = curve + jnp.sum(dir_cov * cov_terms, axis=1, keepdims=True)
        cc[0, :, :C] = cov_terms
        cc[1] = jnp.broadcast_to(curve, (R, 128))
        last = it + 1 == ITERS
        reduce = to_blk(row_blk + 2, lambda j: cc, lambda m: cc_b.at[it, m])
        if not last:
            reduce += to_blk(row_blk + 3, lambda j: p_snd.at[j], lambda m: p_rcv.at[it, m])
            reduce += to_next(it, lambda j: q_snd.at[j], lambda m: q_rcv.at[it, m])
        start_all(reduce)
        cc_b[it, me_b] = cc[...]
        if not last:
            p_rcv[it, me_b] = p_snd[me_b]
        wait_all(reduce)
        cs[...] = jnp.sum(cc_b[it], axis=0)
        share = to_day(row_day + 2, lambda g: cs, lambda m: cc_d.at[it, m])
        if not last:
            for t in range(dl):
                image = jnp.sum(p_rcv[it, :, t], axis=0) + ahead[t]
                if t == 0:
                    image = image + jnp.sum(q_rcv[it], axis=0)
                for g in range(D):
                    x_snd[g, t] = image[g * Rd : (g + 1) * Rd]
            share += to_day(row_day + 3, lambda g: x_snd.at[g], lambda m: x_rcv.at[it + 1, m])
        start_all(share)
        cc_d[it, me_d] = cs[...]
        if not last:
            x_rcv[it + 1, me_d] = x_snd[me_d]
        wait_all(share)
        summed = jnp.sum(cc_d[it], axis=0)
        prior_dir = prior[...] * dir_cov
        image_cov = summed[0, :, :C] + prior_dir
        curvature = summed[1, :, 0:1] + jnp.sum(dir_cov * prior_dir, axis=1, keepdims=True)
        step = norm_now / curvature
        for t in range(dl):
            add = step * dirs[it, me_b, t]
            field_out[t] = add if it == 0 else field_out[t] + add
        sol_cov = sol_cov + step * dir_cov
        if not last:
            resid_cov = resid_cov - step * image_cov
            wide = jnp.broadcast_to(step, (R, 128))
            for g in range(D):
                stepd[g] = wide[g * Rd : (g + 1) * Rd]
            own_step = stepd[me_d][:, 0:1]
            for g in range(D):
                for t in range(dl):
                    resid[g, t] = resid[g, t] - own_step * x_rcv[it + 1, g, t]
        row_day += 4
        row_blk += 4
    cov_out[...] = sol_cov


def on_device(
    D, B,
    diag_blocks, off_blocks, leakage, obs_count, obs_triangle, obs_bary, obs_prec, obs_value,
    covariates, triangles, prior_prec, probes, probes_cov,
):
    dl, n, S = diag_blocks.shape
    J = obs_triangle.shape[1]
    C = covariates.shape[0]
    R = probes.shape[0] + 1
    Rd = R // D
    slot_index = lax.broadcasted_iota(jnp.int32, obs_triangle.shape, 1) + lax.axis_index("blk") * J
    slot_weight = jnp.where(slot_index < obs_count[:, None], obs_prec, jnp.zeros_like(obs_prec))
    vert = jnp.moveaxis(triangles[:, obs_triangle], 0, 2)
    bary = jnp.moveaxis(obs_bary / jnp.sum(obs_bary, axis=0, keepdims=True), 0, 2)
    cov = jnp.moveaxis(covariates, 0, 1)
    padded = jnp.moveaxis(jnp.concatenate([jnp.zeros_like(probes[:1]), probes], axis=0), 0, 1)
    pcov = jnp.concatenate([jnp.zeros_like(probes_cov[:1]), probes_cov], axis=0)
    vm = pltpu.VMEM
    rows = 2 * dl * n
    rows_blk = 2 + 4 * ITERS
    rows_day = 4 + 4 * ITERS
    scratch = [
        vm((rows, S), BF16), vm((rows, S), BF16), vm((dl, J, S), BF16), vm((dl, J, S), BF16),
        vm((SLOTS, CHUNK, S), F32), pltpu.SemaphoreType.DMA((SLOTS,)),
        vm((dl, 8, S), F32), vm((dl, n), F32), vm((D, dl, n), F32), vm((D, dl, n), F32),
        vm((B, dl, 8, n), F32), vm((B, dl, 8, n), F32), vm((8, 128), F32), vm((B, 8, 128), F32),
        vm((8, 128), F32), vm((D, 8, 128), F32),
        vm((D, dl, Rd, n), F32), vm((ITERS, D, dl, Rd, n), F32), vm((D, dl, Rd, n), F32),
        vm((D * dl + 1, Rd, n), F32), vm((ITERS, D, dl + 1, Rd, n), F32),
        vm((Rd, 128), F32), vm((ITERS, D, Rd, 128), F32), vm((R, 128), F32),
        vm((ITERS, B, R, 128), F32), vm((dl + 1, R, n), F32), vm((ITERS, B, dl + 1, R, n), F32),
        vm((ITERS, B, dl + 1, R, n), F32), vm((dl + 1, 2 * R, S), BF16), vm((dl, 2 * R, n), BF16),
        vm((dl, R, S), F32), vm((dl, R, S), F32), vm((dl, R, n), F32),
        vm((B, dl, R, n), F32), vm((ITERS - 1, B, dl, R, n), F32),
        vm((B, R, n), F32), vm((ITERS - 1, B, R, n), F32),
        vm((2, R, 128), F32), vm((ITERS, B, 2, R, 128), F32), vm((2, R, 128), F32),
        vm((ITERS, D, 2, R, 128), F32), vm((D, Rd, 128), F32),
        pltpu.SemaphoreType.DMA((2, rows_blk, B)), pltpu.SemaphoreType.DMA((2, rows_day, D)),
        pltpu.SemaphoreType.DMA((2, ITERS - 1, B)),
    ]
    anywhere = pl.BlockSpec(memory_space=pltpu.HBM)
    inside = pl.BlockSpec(memory_space=pltpu.VMEM)
    field, out_cov = pl.pallas_call(
        functools.partial(kernel, D, B, R, dl, n, J, C),
        out_shape=(jax.ShapeDtypeStruct((dl, R, n), F32), jax.ShapeDtypeStruct((R, C), F32)),
        in_specs=[anywhere] * 2 + [inside] * 9,
        out_specs=(inside, inside),
        scratch_shapes=scratch,
        compiler_params=pltpu.CompilerParams(
            collective_id=0, has_side_effects=True, vmem_limit_bytes=60 * 1024 * 1024
        ),
    )(
        diag_blocks.reshape(dl * n, S), off_blocks.reshape(dl * n, S), vert, bary, cov,
        slot_weight[:, None], (slot_weight * obs_value)[:, None], leakage, padded, pcov,
        prior_prec[None],
    )
    return (jnp.moveaxis(field, 0, 1), out_cov)


def solution(mesh):
    in_specs = (
        P("day", "blk", None),
        P("day", "blk", None),
        P("day", "blk"),
        P("day"),
        P("day", "blk"),
        P(None, "day", "blk"),
        P("day", "blk"),
        P("day", "blk"),
        P(None, "day", "blk"),
        P(),
        P(),
        P(None, "day", "blk"),
        P(),
    )
    out_specs = (P(None, "day", "blk"), P())
    body = functools.partial(on_device, mesh.shape["day"], mesh.shape["blk"])
    return jax.shard_map(
        body, mesh=mesh, in_specs=in_specs, out_specs=out_specs, check_vma=False
    )
```

```python
import functools
import jax
import jax.numpy as jnp
from jax import lax
from jax.experimental import pallas as pl
from jax.experimental.pallas import tpu as pltpu
from jax.sharding import PartitionSpec as P

ITERS = 3
COLS = 256
CHUNK = 64
SLOTS = 8
MESH = pl.DeviceIdType.MESH
F32 = jnp.float32
BF16 = jnp.bfloat16


def split(x):
    hi = x.astype(BF16)
    return hi, (x - hi.astype(F32)).astype(BF16)


def nn(a, b):
    return jnp.dot(a, b, preferred_element_type=F32)


def nt(a, b, precision=None):
    return lax.dot_general(
        a, b, (((1,), (1,)), ((), ())), preferred_element_type=F32, precision=precision
    )


def kernel(
    D, B, R, dl, n, J, C,
    diag, off, vert, bary, cov_in, slotw, value, leak, probes, pcov, prior,
    field_out, cov_out,
    mhi, mlo, ahi, alo, stage, stage_sem,
    dacc, own_dom, leak_all, dom_all, g_snd, g_rcv, gc_snd, gc_rcv, gcd_snd, gcd_rcv,
    cov, rawd, rawb, x_snd, x_rcv, resid, pre, pre_rcv, npart, n_rcv, ncol, nb_rcv, pre_own, pre_full,
    dirs, dhl, ohl, part, behind, ahead, p_snd, p_rcv, q_snd, q_rcv, cc, cc_b, cs, cc_d, stepd,
    sem_blk, sem_day, sem_next,
):
    S = n * B
    T = D * dl
    Rd = R // D
    me_d = lax.axis_index("day")
    me_b = lax.axis_index("blk")

    def at_blk(k):
        return lax.rem(me_b + k, B)

    def at_day(k):
        return lax.rem(me_d + k, D)

    def start_all(copies):
        for c in copies:
            c.start()

    def wait_all(copies):
        for c in copies:
            c.wait()

    def to_blk(row, src, dst):
        return [
            pltpu.make_async_remote_copy(
                src_ref=src(at_blk(k)), dst_ref=dst(me_b),
                send_sem=sem_blk.at[0, row, k], recv_sem=sem_blk.at[1, row, k],
                device_id={"blk": at_blk(k)}, device_id_type=MESH,
            )
            for k in range(1, B)
        ]

    def to_day(row, src, dst):
        return [
            pltpu.make_async_remote_copy(
                src_ref=src(at_day(k)), dst_ref=dst(me_d),
                send_sem=sem_day.at[0, row, k], recv_sem=sem_day.at[1, row, k],
                device_id={"day": at_day(k)}, device_id_type=MESH,
            )
            for k in range(1, D)
        ]

    def to_next(row, src, dst):
        return [
            pltpu.make_async_remote_copy(
                src_ref=src(at_blk(k)), dst_ref=dst(me_b),
                send_sem=sem_next.at[0, row, k], recv_sem=sem_next.at[1, row, k],
                device_id={"day": at_day(1), "blk": at_blk(k)}, device_id_type=MESH,
            )
            for k in range(B)
        ]

    def load(mat, q, slot):
        return pltpu.make_async_copy(
            mat.at[pl.ds(pl.multiple_of(q * CHUNK, CHUNK), CHUNK)], stage.at[slot], stage_sem.at[slot]
        )

    total = dl * n // CHUNK
    per_day = n // CHUNK
    for s in range(min(SLOTS, total)):
        load(diag, s, s).start()

    barrier = pltpu.get_barrier_semaphore()
    for k in range(1, B):
        pl.semaphore_signal(barrier, inc=1, device_id={"blk": at_blk(k)}, device_id_type=MESH)
        pl.semaphore_signal(
            barrier, inc=1, device_id={"day": at_day(D - 1), "blk": at_blk(k)}, device_id_type=MESH
        )
    for k in range(1, D):
        pl.semaphore_signal(barrier, inc=1, device_id={"day": at_day(k)}, device_id_type=MESH)

    for t in range(dl):
        cov[t] = cov_in[:, t, :]
        corner = [vert[k, t : t + 1, :] for k in range(3)]
        raw = [bary[k, t : t + 1, :] for k in range(3)]
        scale = raw[0] + raw[1] + raw[2]
        share_of = [x / scale for x in raw]

        def build(c, carry):
            nodes = pl.ds(pl.multiple_of(c * COLS, COLS), COLS)
            node = lax.broadcasted_iota(jnp.int32, (COLS, J), 0) + c * COLS
            acc = jnp.zeros((COLS, J), F32)
            for k in range(3):
                acc = acc + jnp.where(corner[k] == node, share_of[k], 0.0)
            hi, lo = split(acc)
            ahi[t, nodes] = hi
            alo[t, nodes] = lo
            return carry

        lax.fori_loop(0, S // COLS, build, 0)

    pl.semaphore_wait(barrier, 2 * (B - 1) + D - 1)

    gc = jnp.zeros((8, C), F32)
    for t in range(dl):
        w8 = jnp.broadcast_to(slotw[t : t + 1] * value[t : t + 1], (8, J))
        gc = gc + nt(w8, cov[t], lax.Precision.HIGHEST)
        whi, wlo = split(w8)
        w2 = jnp.concatenate([whi.astype(F32), wlo.astype(F32)], axis=0).astype(BF16)

        def grad(c, carry):
            cols = pl.ds(pl.multiple_of(c * COLS, COLS), COLS)
            g = nt(w2, ahi[t, cols])
            part[t, 0:8, cols] = g[:8] + g[8:] + nt(w2, alo[t, cols])[:8]
            return carry

        lax.fori_loop(0, S // COLS, grad, 0)
        for j in range(B):
            g_snd[j, t] = part[t, 0:8, j * n : (j + 1) * n]
    gc_snd[...] = jnp.zeros_like(gc_snd)
    gc_snd[:, :C] = gc
    cc[...] = jnp.zeros_like(cc)
    first = to_blk(0, lambda j: g_snd.at[j], lambda m: g_rcv.at[m])
    first += to_blk(1, lambda j: gc_snd, lambda m: gc_rcv.at[m])
    first_leak = to_day(0, lambda g: leak, lambda m: leak_all.at[m])
    start_all(first + first_leak)
    g_rcv[me_b] = g_snd[me_b]
    gc_rcv[me_b] = gc_snd[...]
    leak_all[me_d] = leak[...]

    def convert(mat, base, want_diagonal):
        def one(q, carry):
            slot = lax.rem(q, SLOTS)
            load(mat, q, slot).wait()
            x = stage[slot]
            hi, lo = split(x)
            rows = pl.ds(pl.multiple_of(base + q * CHUNK, CHUNK), CHUNK)
            mhi[rows] = hi
            mlo[rows] = lo
            if want_diagonal:
                first_row = me_b * n + lax.rem(q, per_day) * CHUNK
                gap = lax.broadcasted_iota(jnp.int32, (CHUNK, S), 1) - lax.broadcasted_iota(
                    jnp.int32, (CHUNK, S), 0
                )
                picked = jnp.where(gap == first_row, x, 0.0)
                t = q // per_day
                dacc[t] = dacc[t] + jnp.sum(picked.reshape(CHUNK // 8, 8, S), axis=0)

            @pl.when(q + SLOTS < total)
            def _():
                load(mat, q + SLOTS, slot).start()

            return carry

        lax.fori_loop(0, total, one, 0)

    dacc[...] = jnp.zeros_like(dacc)
    convert(diag, 0, True)
    for s in range(min(SLOTS, total)):
        load(off, s, s).start()
    for t in range(dl):
        row = jnp.sum(dacc[t], axis=0, keepdims=True)
        acc = row[:, :n]
        for j in range(1, B):
            acc = acc + row[:, j * n : (j + 1) * n]
        own_dom[t : t + 1] = acc
    first_dom = to_day(1, lambda g: own_dom, lambda m: dom_all.at[m])
    start_all(first_dom)
    dom_all[me_d] = own_dom[...]

    wait_all(first)
    g_own = jnp.sum(g_rcv[...], axis=0)
    gcd_snd[...] = jnp.sum(gc_rcv[...], axis=0)
    for t in range(dl):
        pre_own[t, 0:1] = g_own[t, 0:1]
        pre_own[t, 1:R] = probes[:, t, :]
        r = pre_own[t]
        for g in range(D):
            x_snd[g, t] = r[g * Rd : (g + 1) * Rd]
    move = to_day(2, lambda g: x_snd.at[g], lambda m: x_rcv.at[0, m])
    move += to_day(3, lambda g: gcd_snd, lambda m: gcd_rcv.at[m])
    start_all(move)
    x_rcv[0, me_d] = x_snd[me_d]
    gcd_rcv[me_d] = gcd_snd[...]
    convert(off, dl * n, False)
    wait_all(first_leak + first_dom + move)
    ncol[0:1] = jnp.sum(gcd_rcv[...], axis=0)[0:1]
    ncol[1:R, 0:C] = pcov[...]
    resid_cov = ncol[:, 0:C]
    resid[...] = x_rcv[0]
    pre[T] = jnp.zeros((Rd, n), F32)

    live = jnp.where(me_d == D - 1, 0.0, 1.0).astype(F32)
    norm_now = None
    sol_cov = jnp.zeros((R, C), F32)
    dir_cov = None
    row_day = 4
    row_blk = 2
    for it in range(ITERS):
        running = jnp.zeros((Rd, n), F32)
        for t in range(T):
            decay = 1.0 - leak_all[t // dl, t % dl : t % dl + 1]
            running = resid[t // dl, t % dl] + decay * running
            pre[t] = running / dom_all[t // dl, t % dl : t % dl + 1]
        running = pre[T - 1]
        norm_part = resid[D - 1, dl - 1] * running
        for t in range(T - 2, -1, -1):
            u = t + 1
            decay = 1.0 - leak_all[u // dl, u % dl : u % dl + 1]
            running = pre[t] + decay * running
            pre[t] = running
            norm_part = norm_part + resid[t // dl, t % dl] * running
        npart[...] = jnp.broadcast_to(jnp.sum(norm_part, axis=1, keepdims=True), (Rd, 128))
        back = to_day(
            row_day, lambda g: pre.at[pl.ds(g * dl, dl + 1)], lambda m: pre_rcv.at[it, m]
        )
        back += to_day(row_day + 1, lambda g: npart, lambda m: n_rcv.at[it, m])
        start_all(back)
        for t in range(dl + 1):
            pre_rcv[it, me_d, t] = pre[me_d * dl + t]
        n_rcv[it, me_d] = npart[...]
        wait_all(back)
        for g in range(D):
            for t in range(dl + 1):
                pre_own[t, g * Rd : (g + 1) * Rd] = pre_rcv[it, g, t]
            ncol[g * Rd : (g + 1) * Rd] = n_rcv[it, g]
        norms = to_blk(row_blk + 1, lambda j: ncol, lambda m: nb_rcv.at[it, m])
        spread_out = to_blk(row_blk, lambda j: pre_own, lambda m: pre_full.at[it, m])
        start_all(norms + spread_out)
        pre_full[it, me_b] = pre_own[...]
        nb_rcv[it, me_b] = ncol[...]
        last = it + 1 == ITERS

        for t in range(dl):
            hi, lo = split(pre_own[t])
            ohl[t, 0:R] = hi
            ohl[t, R : 2 * R] = lo

            def columns(c, carry):
                cols = pl.ds(pl.multiple_of(c * COLS, COLS), COLS)
                rows = slice(t * n, (t + 1) * n)
                orows = slice((dl + t) * n, (dl + t + 1) * n)
                dv = ohl[t]
                x = nn(dv, mhi[rows, cols])
                rawd[t, :, cols] = x[:R] + x[R:] + nn(dv[:R], mlo[rows, cols])
                x = nn(dv, mhi[orows, cols])
                rawb[t, :, cols] = x[:R] + x[R:] + nn(dv[:R], mlo[orows, cols])
                return carry

            lax.fori_loop(0, S // COLS, columns, 0)
        wait_all(norms)
        norm_next = jnp.sum(nb_rcv[it], axis=0)[:, 0:1] + jnp.sum(
            resid_cov * resid_cov, axis=1, keepdims=True
        )
        if it == 0:
            dir_cov = resid_cov
            part[...] = rawd[...]
            behind[...] = rawb[...]
        else:
            beta = norm_next / norm_now
            dir_cov = resid_cov + beta * dir_cov
            for t in range(dl):
                part[t] = rawd[t] + beta * part[t]
                behind[t] = rawb[t] + beta * behind[t]
        norm_now = norm_next
        ahead_send = []
        if not last:
            for j in range(B):
                q_snd[j] = behind[dl - 1, :, j * n : (j + 1) * n] * live
            ahead_send = to_next(it, lambda j: q_snd.at[j], lambda m: q_rcv.at[it, m])
            start_all(ahead_send)
        wait_all(spread_out)
        for j in range(B):
            for t in range(dl + 1):
                d = pre_full[it, j, t]
                if it > 0:
                    d = d + beta * dirs[it - 1, j, t]
                dirs[it, j, t] = d
                hi, lo = split(d)
                dhl[t, 0:R, j * n : (j + 1) * n] = hi
                dhl[t, R : 2 * R, j * n : (j + 1) * n] = lo

        curve = jnp.zeros((R, 1), F32)
        cov_terms = jnp.zeros((R, C), F32)
        for t in range(dl):
            both = nn(dhl[t], ahi[t])
            predictor = both[:R] + both[R:] + nn(dhl[t, 0:R], alo[t])
            predictor = predictor + jnp.dot(
                dir_cov, cov[t], preferred_element_type=F32, precision=lax.Precision.HIGHEST
            )
            weighted = slotw[t : t + 1] * predictor
            curve = curve + jnp.sum(weighted * predictor, axis=1, keepdims=True)
            if not last:
                cov_terms = cov_terms + nt(weighted, cov[t], lax.Precision.HIGHEST)
                whi, wlo = split(weighted)
                w2 = jnp.concatenate([whi, wlo], axis=0)

                def observed(c, carry):
                    cols = pl.ds(pl.multiple_of(c * COLS, COLS), COLS)
                    x = nt(w2, ahi[t, cols])
                    rawd[t, :, cols] = x[:R] + x[R:] + nt(whi, alo[t, cols])
                    return carry

                lax.fori_loop(0, S // COLS, observed, 0)
        acc = [jnp.zeros((R, n), F32) for _ in range(2)]
        for j in range(B):
            piece = slice(j * n, (j + 1) * n)
            for t in range(dl):
                p = part[t, :, piece]
                q = behind[t, :, piece]
                acc[0] = acc[0] + p * dirs[it, j, t]
                acc[1] = acc[1] + q * dirs[it, j, t + 1]
                if not last:
                    p = p + rawd[t, :, piece]
                    if t > 0:
                        p = p + behind[t - 1, :, piece]
                    p_snd[j, t] = p
        curve = curve + jnp.sum(acc[0] + 2.0 * acc[1], axis=1, keepdims=True)
        cc[0, :, :C] = cov_terms
        cc[1] = jnp.broadcast_to(curve, (R, 128))
        reduce = to_blk(row_blk + 2, lambda j: cc, lambda m: cc_b.at[it, m])
        if not last:
            reduce += to_blk(row_blk + 3, lambda j: p_snd.at[j], lambda m: p_rcv.at[it, m])
        start_all(reduce)
        cc_b[it, me_b] = cc[...]
        if not last:
            p_rcv[it, me_b] = p_snd[me_b]
            for t in range(dl):
                x = nt(dhl[t + 1], mhi[(dl + t) * n : (dl + t + 1) * n])
                ahead[t] = (
                    x[:R] + x[R:] + nt(dhl[t + 1, 0:R], mlo[(dl + t) * n : (dl + t + 1) * n])
                )
        wait_all(reduce + ahead_send)
        cs[...] = jnp.sum(cc_b[it], axis=0)
        share = to_day(row_day + 2, lambda g: cs, lambda m: cc_d.at[it, m])
        if not last:
            for t in range(dl):
                image = jnp.sum(p_rcv[it, :, t], axis=0) + ahead[t]
                if t == 0:
                    image = image + jnp.sum(q_rcv[it], axis=0)
                for g in range(D):
                    x_snd[g, t] = image[g * Rd : (g + 1) * Rd]
            share += to_day(row_day + 3, lambda g: x_snd.at[g], lambda m: x_rcv.at[it + 1, m])
        start_all(share)
        cc_d[it, me_d] = cs[...]
        if not last:
            x_rcv[it + 1, me_d] = x_snd[me_d]
        wait_all(share)
        summed = jnp.sum(cc_d[it], axis=0)
        prior_dir = prior[...] * dir_cov
        image_cov = summed[0, :, :C] + prior_dir
        curvature = summed[1, :, 0:1] + jnp.sum(dir_cov * prior_dir, axis=1, keepdims=True)
        step = norm_now / curvature
        for t in range(dl):
            add = step * dirs[it, me_b, t]
            field_out[t] = add if it == 0 else field_out[t] + add
        sol_cov = sol_cov + step * dir_cov
        if not last:
            resid_cov = resid_cov - step * image_cov
            wide = jnp.broadcast_to(step, (R, 128))
            for g in range(D):
                stepd[g] = wide[g * Rd : (g + 1) * Rd]
            own_step = stepd[me_d][:, 0:1]
            for g in range(D):
                for t in range(dl):
                    resid[g, t] = resid[g, t] - own_step * x_rcv[it + 1, g, t]
        row_day += 4
        row_blk += 4
    cov_out[...] = sol_cov


def on_device(
    D, B,
    diag_blocks, off_blocks, leakage, obs_count, obs_triangle, obs_bary, obs_prec, obs_value,
    covariates, triangles, prior_prec, probes, probes_cov,
):
    dl, n, S = diag_blocks.shape
    J = obs_triangle.shape[1]
    C = covariates.shape[0]
    R = probes.shape[0] + 1
    Rd = R // D
    slot_index = lax.broadcasted_iota(jnp.int32, obs_triangle.shape, 1) + lax.axis_index("blk") * J
    slot_weight = jnp.where(slot_index < obs_count[:, None], obs_prec, jnp.zeros_like(obs_prec))
    vert = triangles[:, obs_triangle]
    vm = pltpu.VMEM
    rows = 2 * dl * n
    rows_blk = 2 + 4 * ITERS
    rows_day = 4 + 4 * ITERS
    scratch = [
        vm((rows, S), BF16), vm((rows, S), BF16), vm((dl, S, J), BF16), vm((dl, S, J), BF16),
        vm((SLOTS, CHUNK, S), F32), pltpu.SemaphoreType.DMA((SLOTS,)),
        vm((dl, 8, S), F32), vm((dl, n), F32), vm((D, dl, n), F32), vm((D, dl, n), F32),
        vm((B, dl, 8, n), F32), vm((B, dl, 8, n), F32), vm((8, 128), F32), vm((B, 8, 128), F32),
        vm((8, 128), F32), vm((D, 8, 128), F32),
        vm((dl, C, J), F32), vm((dl, R, S), F32), vm((dl, R, S), F32),
        vm((D, dl, Rd, n), F32), vm((ITERS, D, dl, Rd, n), F32), vm((D, dl, Rd, n), F32),
        vm((D * dl + 1, Rd, n), F32), vm((ITERS, D, dl + 1, Rd, n), F32),
        vm((Rd, 128), F32), vm((ITERS, D, Rd, 128), F32), vm((R, 128), F32),
        vm((ITERS, B, R, 128), F32), vm((dl + 1, R, n), F32), vm((ITERS, B, dl + 1, R, n), F32),
        vm((ITERS, B, dl + 1, R, n), F32), vm((dl + 1, 2 * R, S), BF16), vm((dl, 2 * R, n), BF16),
        vm((dl, R, S), F32), vm((dl, R, S), F32), vm((dl, R, n), F32),
        vm((B, dl, R, n), F32), vm((ITERS - 1, B, dl, R, n), F32),
        vm((B, R, n), F32), vm((ITERS - 1, B, R, n), F32),
        vm((2, R, 128), F32), vm((ITERS, B, 2, R, 128), F32), vm((2, R, 128), F32),
        vm((ITERS, D, 2, R, 128), F32), vm((D, Rd, 128), F32),
        pltpu.SemaphoreType.DMA((2, rows_blk, B)), pltpu.SemaphoreType.DMA((2, rows_day, D)),
        pltpu.SemaphoreType.DMA((2, ITERS - 1, B)),
    ]
    anywhere = pl.BlockSpec(memory_space=pltpu.HBM)
    inside = pl.BlockSpec(memory_space=pltpu.VMEM)
    field, out_cov = pl.pallas_call(
        functools.partial(kernel, D, B, R, dl, n, J, C),
        out_shape=(jax.ShapeDtypeStruct((dl, R, n), F32), jax.ShapeDtypeStruct((R, C), F32)),
        in_specs=[anywhere] * 2 + [inside] * 9,
        out_specs=(inside, inside),
        scratch_shapes=scratch,
        compiler_params=pltpu.CompilerParams(
            collective_id=0, has_side_effects=True, vmem_limit_bytes=60 * 1024 * 1024
        ),
    )(
        diag_blocks.reshape(dl * n, S), off_blocks.reshape(dl * n, S), vert, obs_bary, covariates,
        slot_weight, obs_value, leakage, probes, probes_cov, prior_prec[None],
    )
    return (jnp.moveaxis(field, 0, 1), out_cov)


def solution(mesh):
    in_specs = (
        P("day", "blk", None),
        P("day", "blk", None),
        P("day", "blk"),
        P("day"),
        P("day", "blk"),
        P(None, "day", "blk"),
        P("day", "blk"),
        P("day", "blk"),
        P(None, "day", "blk"),
        P(),
        P(),
        P(None, "day", "blk"),
        P(),
    )
    out_specs = (P(None, "day", "blk"), P())
    body = functools.partial(on_device, mesh.shape["day"], mesh.shape["blk"])
    return jax.shard_map(
        body, mesh=mesh, in_specs=in_specs, out_specs=out_specs, check_vma=False
    )
```

```python
import functools
import jax
import jax.numpy as jnp
from jax import lax
from jax.experimental import pallas as pl
from jax.experimental.pallas import tpu as pltpu
from jax.sharding import PartitionSpec as P

ITERS = 3
COLS = 256
CHUNK = 64
SLOTS = 8
MESH = pl.DeviceIdType.MESH
F32 = jnp.float32
BF16 = jnp.bfloat16


def split(x):
    hi = x.astype(BF16)
    return hi, (x - hi.astype(F32)).astype(BF16)


def nn(a, b):
    return jnp.dot(a, b, preferred_element_type=F32)


def nt(a, b, precision=None):
    return lax.dot_general(
        a, b, (((1,), (1,)), ((), ())), preferred_element_type=F32, precision=precision
    )


def kernel(
    D, B, R, dl, n, J, C,
    diag, off, vert, bary, cov_in, slotw, value, leak, probes, pcov, prior,
    field_out, cov_out,
    mhi, mlo, ahi, alo, stage, stage_sem,
    dacc, own_dom, leak_all, dom_all, g_snd, g_rcv, gc_snd, gc_rcv, gcd_snd, gcd_rcv,
    cov, sol, rawd, rawb, x_snd, x_rcv, resid, pre, pre_rcv, npart, n_rcv, ncol, nb_rcv, pre_own, pre_full,
    dirs, dhl, ohl, part, behind, ahead, p_snd, p_rcv, q_snd, q_rcv, cc, cc_b, cs, cc_d, stepd,
    sem_blk, sem_day, sem_next,
):
    S = n * B
    T = D * dl
    Rd = R // D
    me_d = lax.axis_index("day")
    me_b = lax.axis_index("blk")

    def at_blk(k):
        return lax.rem(me_b + k, B)

    def at_day(k):
        return lax.rem(me_d + k, D)

    def start_all(copies):
        for c in copies:
            c.start()

    def wait_all(copies):
        for c in copies:
            c.wait()

    def to_blk(row, src, dst):
        return [
            pltpu.make_async_remote_copy(
                src_ref=src(at_blk(k)), dst_ref=dst(me_b),
                send_sem=sem_blk.at[0, row, k], recv_sem=sem_blk.at[1, row, k],
                device_id={"blk": at_blk(k)}, device_id_type=MESH,
            )
            for k in range(1, B)
        ]

    def to_day(row, src, dst):
        return [
            pltpu.make_async_remote_copy(
                src_ref=src(at_day(k)), dst_ref=dst(me_d),
                send_sem=sem_day.at[0, row, k], recv_sem=sem_day.at[1, row, k],
                device_id={"day": at_day(k)}, device_id_type=MESH,
            )
            for k in range(1, D)
        ]

    def to_next(row, src, dst):
        return [
            pltpu.make_async_remote_copy(
                src_ref=src(at_blk(k)), dst_ref=dst(me_b),
                send_sem=sem_next.at[0, row, k], recv_sem=sem_next.at[1, row, k],
                device_id={"day": at_day(1), "blk": at_blk(k)}, device_id_type=MESH,
            )
            for k in range(B)
        ]

    def load(mat, q, slot):
        return pltpu.make_async_copy(
            mat.at[pl.ds(pl.multiple_of(q * CHUNK, CHUNK), CHUNK)], stage.at[slot], stage_sem.at[slot]
        )

    total = dl * n // CHUNK
    per_day = n // CHUNK
    for s in range(min(SLOTS, total)):
        load(diag, s, s).start()

    barrier = pltpu.get_barrier_semaphore()
    for k in range(1, B):
        pl.semaphore_signal(barrier, inc=1, device_id={"blk": at_blk(k)}, device_id_type=MESH)
        pl.semaphore_signal(
            barrier, inc=1, device_id={"day": at_day(D - 1), "blk": at_blk(k)}, device_id_type=MESH
        )
    for k in range(1, D):
        pl.semaphore_signal(barrier, inc=1, device_id={"day": at_day(k)}, device_id_type=MESH)

    for t in range(dl):
        cov[t] = cov_in[:, t, :]
        corner = [vert[k, t : t + 1, :] for k in range(3)]
        raw = [bary[k, t : t + 1, :] for k in range(3)]
        scale = raw[0] + raw[1] + raw[2]
        share_of = [x / scale for x in raw]

        def build(c, carry):
            nodes = pl.ds(pl.multiple_of(c * COLS, COLS), COLS)
            node = lax.broadcasted_iota(jnp.int32, (COLS, J), 0) + c * COLS
            acc = jnp.zeros((COLS, J), F32)
            for k in range(3):
                acc = acc + jnp.where(corner[k] == node, share_of[k], 0.0)
            hi, lo = split(acc)
            ahi[t, nodes] = hi
            alo[t, nodes] = lo
            return carry

        lax.fori_loop(0, S // COLS, build, 0)

    pl.semaphore_wait(barrier, 2 * (B - 1) + D - 1)

    gc = jnp.zeros((8, C), F32)
    for t in range(dl):
        w8 = jnp.broadcast_to(slotw[t : t + 1] * value[t : t + 1], (8, J))
        gc = gc + nt(w8, cov[t], lax.Precision.HIGHEST)
        whi, wlo = split(w8)
        w2 = jnp.concatenate([whi.astype(F32), wlo.astype(F32)], axis=0).astype(BF16)

        def grad(c, carry):
            cols = pl.ds(pl.multiple_of(c * COLS, COLS), COLS)
            g = nt(w2, ahi[t, cols])
            part[t, 0:8, cols] = g[:8] + g[8:] + nt(w2, alo[t, cols])[:8]
            return carry

        lax.fori_loop(0, S // COLS, grad, 0)
        for j in range(B):
            g_snd[j, t] = part[t, 0:8, j * n : (j + 1) * n]
    gc_snd[...] = jnp.zeros_like(gc_snd)
    gc_snd[:, :C] = gc
    cc[...] = jnp.zeros_like(cc)
    first = to_blk(0, lambda j: g_snd.at[j], lambda m: g_rcv.at[m])
    first += to_blk(1, lambda j: gc_snd, lambda m: gc_rcv.at[m])
    first_leak = to_day(0, lambda g: leak, lambda m: leak_all.at[m])
    start_all(first + first_leak)
    g_rcv[me_b] = g_snd[me_b]
    gc_rcv[me_b] = gc_snd[...]
    leak_all[me_d] = leak[...]

    def convert(mat, base, want_diagonal):
        def one(q, carry):
            slot = lax.rem(q, SLOTS)
            load(mat, q, slot).wait()
            x = stage[slot]
            hi, lo = split(x)
            rows = pl.ds(pl.multiple_of(base + q * CHUNK, CHUNK), CHUNK)
            mhi[rows] = hi
            mlo[rows] = lo
            if want_diagonal:
                first_row = me_b * n + lax.rem(q, per_day) * CHUNK
                gap = lax.broadcasted_iota(jnp.int32, (CHUNK, S), 1) - lax.broadcasted_iota(
                    jnp.int32, (CHUNK, S), 0
                )
                picked = jnp.where(gap == first_row, x, 0.0)
                t = q // per_day
                dacc[t] = dacc[t] + jnp.sum(picked.reshape(CHUNK // 8, 8, S), axis=0)

            @pl.when(q + SLOTS < total)
            def _():
                load(mat, q + SLOTS, slot).start()

            return carry

        lax.fori_loop(0, total, one, 0)

    dacc[...] = jnp.zeros_like(dacc)
    convert(diag, 0, True)
    for s in range(min(SLOTS, total)):
        load(off, s, s).start()
    for t in range(dl):
        row = jnp.sum(dacc[t], axis=0, keepdims=True)
        acc = row[:, :n]
        for j in range(1, B):
            acc = acc + row[:, j * n : (j + 1) * n]
        own_dom[t : t + 1] = acc
    first_dom = to_day(1, lambda g: own_dom, lambda m: dom_all.at[m])
    start_all(first_dom)
    dom_all[me_d] = own_dom[...]

    wait_all(first)
    g_own = jnp.sum(g_rcv[...], axis=0)
    gcd_snd[...] = jnp.sum(gc_rcv[...], axis=0)
    for t in range(dl):
        pre_own[t, 0:1] = g_own[t, 0:1]
        pre_own[t, 1:R] = probes[:, t, :]
        r = pre_own[t]
        for g in range(D):
            x_snd[g, t] = r[g * Rd : (g + 1) * Rd]
    move = to_day(2, lambda g: x_snd.at[g], lambda m: x_rcv.at[0, m])
    move += to_day(3, lambda g: gcd_snd, lambda m: gcd_rcv.at[m])
    start_all(move)
    x_rcv[0, me_d] = x_snd[me_d]
    gcd_rcv[me_d] = gcd_snd[...]
    convert(off, dl * n, False)
    wait_all(first_leak + first_dom + move)
    ncol[0:1] = jnp.sum(gcd_rcv[...], axis=0)[0:1]
    ncol[1:R, 0:C] = pcov[...]
    resid_cov = ncol[:, 0:C]
    resid[...] = x_rcv[0]
    pre[T] = jnp.zeros((Rd, n), F32)

    live = jnp.where(me_d == D - 1, 0.0, 1.0).astype(F32)
    norm_now = None
    sol_cov = jnp.zeros((R, C), F32)
    dir_cov = None
    row_day = 4
    row_blk = 2
    for it in range(ITERS):
        running = jnp.zeros((Rd, n), F32)
        for t in range(T):
            decay = 1.0 - leak_all[t // dl, t % dl : t % dl + 1]
            running = resid[t // dl, t % dl] + decay * running
            pre[t] = running / dom_all[t // dl, t % dl : t % dl + 1]
        running = pre[T - 1]
        norm_part = resid[D - 1, dl - 1] * running
        for t in range(T - 2, -1, -1):
            u = t + 1
            decay = 1.0 - leak_all[u // dl, u % dl : u % dl + 1]
            running = pre[t] + decay * running
            pre[t] = running
            norm_part = norm_part + resid[t // dl, t % dl] * running
        npart[...] = jnp.broadcast_to(jnp.sum(norm_part, axis=1, keepdims=True), (Rd, 128))
        back = to_day(
            row_day, lambda g: pre.at[pl.ds(g * dl, dl + 1)], lambda m: pre_rcv.at[it, m]
        )
        back += to_day(row_day + 1, lambda g: npart, lambda m: n_rcv.at[it, m])
        start_all(back)
        for t in range(dl + 1):
            pre_rcv[it, me_d, t] = pre[me_d * dl + t]
        n_rcv[it, me_d] = npart[...]
        wait_all(back)
        for g in range(D):
            for t in range(dl + 1):
                pre_own[t, g * Rd : (g + 1) * Rd] = pre_rcv[it, g, t]
            ncol[g * Rd : (g + 1) * Rd] = n_rcv[it, g]
        norms = to_blk(row_blk + 1, lambda j: ncol, lambda m: nb_rcv.at[it, m])
        spread_out = to_blk(row_blk, lambda j: pre_own, lambda m: pre_full.at[it, m])
        start_all(norms + spread_out)
        pre_full[it, me_b] = pre_own[...]
        nb_rcv[it, me_b] = ncol[...]
        last = it + 1 == ITERS

        for t in range(dl):
            hi, lo = split(pre_own[t])
            ohl[t, 0:R] = hi
            ohl[t, R : 2 * R] = lo

            def columns(c, carry):
                cols = pl.ds(pl.multiple_of(c * COLS, COLS), COLS)
                rows = slice(t * n, (t + 1) * n)
                orows = slice((dl + t) * n, (dl + t + 1) * n)
                dv = ohl[t]
                x = nn(dv, mhi[rows, cols])
                rawd[t, :, cols] = x[:R] + x[R:] + nn(dv[:R], mlo[rows, cols])
                x = nn(dv, mhi[orows, cols])
                rawb[t, :, cols] = x[:R] + x[R:] + nn(dv[:R], mlo[orows, cols])
                return carry

            lax.fori_loop(0, S // COLS, columns, 0)
        wait_all(norms)
        norm_next = jnp.sum(nb_rcv[it], axis=0)[:, 0:1] + jnp.sum(
            resid_cov * resid_cov, axis=1, keepdims=True
        )
        if it == 0:
            dir_cov = resid_cov
            part[...] = rawd[...]
            behind[...] = rawb[...]
        else:
            beta = norm_next / norm_now
            dir_cov = resid_cov + beta * dir_cov
            for t in range(dl):
                part[t] = rawd[t] + beta * part[t]
                behind[t] = rawb[t] + beta * behind[t]
        norm_now = norm_next
        ahead_send = []
        if not last:
            for j in range(B):
                q_snd[j] = behind[dl - 1, :, j * n : (j + 1) * n] * live
            ahead_send = to_next(it, lambda j: q_snd.at[j], lambda m: q_rcv.at[it, m])
            start_all(ahead_send)
        wait_all(spread_out)
        for j in range(B):
            for t in range(dl + 1):
                d = pre_full[it, j, t]
                if it > 0:
                    d = d + beta * dirs[it - 1, j, t]
                dirs[it, j, t] = d
                hi, lo = split(d)
                dhl[t, 0:R, j * n : (j + 1) * n] = hi
                dhl[t, R : 2 * R, j * n : (j + 1) * n] = lo

        curve = jnp.zeros((R, 1), F32)
        cov_terms = jnp.zeros((R, C), F32)
        for t in range(dl):
            both = nn(dhl[t], ahi[t])
            predictor = both[:R] + both[R:] + nn(dhl[t, 0:R], alo[t])
            predictor = predictor + jnp.dot(
                dir_cov, cov[t], preferred_element_type=F32, precision=lax.Precision.HIGHEST
            )
            weighted = slotw[t : t + 1] * predictor
            curve = curve + jnp.sum(weighted * predictor, axis=1, keepdims=True)
            if not last:
                cov_terms = cov_terms + nt(weighted, cov[t], lax.Precision.HIGHEST)
                whi, wlo = split(weighted)
                w2 = jnp.concatenate([whi, wlo], axis=0)

                def observed(c, carry):
                    cols = pl.ds(pl.multiple_of(c * COLS, COLS), COLS)
                    x = nt(w2, ahi[t, cols])
                    rawd[t, :, cols] = x[:R] + x[R:] + nt(whi, alo[t, cols])
                    return carry

                lax.fori_loop(0, S // COLS, observed, 0)
        acc = [jnp.zeros((R, n), F32) for _ in range(2)]
        for j in range(B):
            piece = slice(j * n, (j + 1) * n)
            for t in range(dl):
                p = part[t, :, piece]
                q = behind[t, :, piece]
                acc[0] = acc[0] + p * dirs[it, j, t]
                acc[1] = acc[1] + q * dirs[it, j, t + 1]
                if not last:
                    p = p + rawd[t, :, piece]
                    if t > 0:
                        p = p + behind[t - 1, :, piece]
                    p_snd[j, t] = p
        curve = curve + jnp.sum(acc[0] + 2.0 * acc[1], axis=1, keepdims=True)
        cc[0, :, :C] = cov_terms
        cc[1] = jnp.broadcast_to(curve, (R, 128))
        reduce = to_blk(row_blk + 2, lambda j: cc, lambda m: cc_b.at[it, m])
        if not last:
            reduce += to_blk(row_blk + 3, lambda j: p_snd.at[j], lambda m: p_rcv.at[it, m])
        start_all(reduce)
        cc_b[it, me_b] = cc[...]
        if not last:
            p_rcv[it, me_b] = p_snd[me_b]
            for t in range(dl):
                x = nt(dhl[t + 1], mhi[(dl + t) * n : (dl + t + 1) * n])
                ahead[t] = (
                    x[:R] + x[R:] + nt(dhl[t + 1, 0:R], mlo[(dl + t) * n : (dl + t + 1) * n])
                )
        wait_all(reduce + ahead_send)
        cs[...] = jnp.sum(cc_b[it], axis=0)
        share = to_day(row_day + 2, lambda g: cs, lambda m: cc_d.at[it, m])
        if not last:
            for t in range(dl):
                image = jnp.sum(p_rcv[it, :, t], axis=0) + ahead[t]
                if t == 0:
                    image = image + jnp.sum(q_rcv[it], axis=0)
                for g in range(D):
                    x_snd[g, t] = image[g * Rd : (g + 1) * Rd]
            share += to_day(row_day + 3, lambda g: x_snd.at[g], lambda m: x_rcv.at[it + 1, m])
        start_all(share)
        cc_d[it, me_d] = cs[...]
        if not last:
            x_rcv[it + 1, me_d] = x_snd[me_d]
        wait_all(share)
        summed = jnp.sum(cc_d[it], axis=0)
        prior_dir = prior[...] * dir_cov
        image_cov = summed[0, :, :C] + prior_dir
        curvature = summed[1, :, 0:1] + jnp.sum(dir_cov * prior_dir, axis=1, keepdims=True)
        step = norm_now / curvature
        for t in range(dl):
            add = step * dirs[it, me_b, t]
            ahead[t] = add if it == 0 else sol[t] + add
            sol[t] = ahead[t]
            if last:
                field_out[:, t, :] = ahead[t]
        sol_cov = sol_cov + step * dir_cov
        if not last:
            resid_cov = resid_cov - step * image_cov
            wide = jnp.broadcast_to(step, (R, 128))
            for g in range(D):
                stepd[g] = wide[g * Rd : (g + 1) * Rd]
            own_step = stepd[me_d][:, 0:1]
            for g in range(D):
                for t in range(dl):
                    resid[g, t] = resid[g, t] - own_step * x_rcv[it + 1, g, t]
        row_day += 4
        row_blk += 4
    cov_out[...] = sol_cov


def on_device(
    D, B,
    diag_blocks, off_blocks, leakage, obs_count, obs_triangle, obs_bary, obs_prec, obs_value,
    covariates, triangles, prior_prec, probes, probes_cov,
):
    dl, n, S = diag_blocks.shape
    J = obs_triangle.shape[1]
    C = covariates.shape[0]
    R = probes.shape[0] + 1
    Rd = R // D
    slot_index = lax.broadcasted_iota(jnp.int32, obs_triangle.shape, 1) + lax.axis_index("blk") * J
    slot_weight = jnp.where(slot_index < obs_count[:, None], obs_prec, jnp.zeros_like(obs_prec))
    vert = triangles[:, obs_triangle]
    vm = pltpu.VMEM
    rows = 2 * dl * n
    rows_blk = 2 + 4 * ITERS
    rows_day = 4 + 4 * ITERS
    scratch = [
        vm((rows, S), BF16), vm((rows, S), BF16), vm((dl, S, J), BF16), vm((dl, S, J), BF16),
        vm((SLOTS, CHUNK, S), F32), pltpu.SemaphoreType.DMA((SLOTS,)),
        vm((dl, 8, S), F32), vm((dl, n), F32), vm((D, dl, n), F32), vm((D, dl, n), F32),
        vm((B, dl, 8, n), F32), vm((B, dl, 8, n), F32), vm((8, 128), F32), vm((B, 8, 128), F32),
        vm((8, 128), F32), vm((D, 8, 128), F32),
        vm((dl, C, J), F32), vm((dl, R, n), F32), vm((dl, R, S), F32), vm((dl, R, S), F32),
        vm((D, dl, Rd, n), F32), vm((ITERS, D, dl, Rd, n), F32), vm((D, dl, Rd, n), F32),
        vm((D * dl + 1, Rd, n), F32), vm((ITERS, D, dl + 1, Rd, n), F32),
        vm((Rd, 128), F32), vm((ITERS, D, Rd, 128), F32), vm((R, 128), F32),
        vm((ITERS, B, R, 128), F32), vm((dl + 1, R, n), F32), vm((ITERS, B, dl + 1, R, n), F32),
        vm((ITERS, B, dl + 1, R, n), F32), vm((dl + 1, 2 * R, S), BF16), vm((dl, 2 * R, n), BF16),
        vm((dl, R, S), F32), vm((dl, R, S), F32), vm((dl, R, n), F32),
        vm((B, dl, R, n), F32), vm((ITERS - 1, B, dl, R, n), F32),
        vm((B, R, n), F32), vm((ITERS - 1, B, R, n), F32),
        vm((2, R, 128), F32), vm((ITERS, B, 2, R, 128), F32), vm((2, R, 128), F32),
        vm((ITERS, D, 2, R, 128), F32), vm((D, Rd, 128), F32),
        pltpu.SemaphoreType.DMA((2, rows_blk, B)), pltpu.SemaphoreType.DMA((2, rows_day, D)),
        pltpu.SemaphoreType.DMA((2, ITERS - 1, B)),
    ]
    anywhere = pl.BlockSpec(memory_space=pltpu.HBM)
    inside = pl.BlockSpec(memory_space=pltpu.VMEM)
    field, out_cov = pl.pallas_call(
        functools.partial(kernel, D, B, R, dl, n, J, C),
        out_shape=(jax.ShapeDtypeStruct((R, dl, n), F32), jax.ShapeDtypeStruct((R, C), F32)),
        in_specs=[anywhere] * 2 + [inside] * 9,
        out_specs=(inside, inside),
        scratch_shapes=scratch,
        compiler_params=pltpu.CompilerParams(
            collective_id=0, has_side_effects=True, vmem_limit_bytes=60 * 1024 * 1024
        ),
    )(
        diag_blocks.reshape(dl * n, S), off_blocks.reshape(dl * n, S), vert, obs_bary, covariates,
        slot_weight, obs_value, leakage, probes, probes_cov, prior_prec[None],
    )
    return (field, out_cov)


def solution(mesh):
    in_specs = (
        P("day", "blk", None),
        P("day", "blk", None),
        P("day", "blk"),
        P("day"),
        P("day", "blk"),
        P(None, "day", "blk"),
        P("day", "blk"),
        P("day", "blk"),
        P(None, "day", "blk"),
        P(),
        P(),
        P(None, "day", "blk"),
        P(),
    )
    out_specs = (P(None, "day", "blk"), P())
    body = functools.partial(on_device, mesh.shape["day"], mesh.shape["blk"])
    return jax.shard_map(
        body, mesh=mesh, in_specs=in_specs, out_specs=out_specs, check_vma=False
    )
```
